256 devices in a mesh: data: 256 (over z, y, x, core).
Axes of the slice: x: 4, y: 4, z: 8, core: 2. Of those that a mesh axis runs over, the one named last changes fastest.
Arguments:
- view_one: bfloat16 [65536, 256], P('data')
- view_two: bfloat16 [65536, 256], P('data')
- protos: bfloat16 [1024, 256], replicated
- valid_mask: int32 [65536], P('data')
Outputs:
- output 1: float32 [65536, 1024], P('data')
- output 2: float32 [65536, 1024], P('data')
- output 3: float32 [], replicated
- output 4: float32 [65536, 256], P('data')
- output 5: float32 [65536, 256], P('data')
- output 6: float32 [1024, 256], replicated
All inputs are finite; a program needn't handle non-finite values.
Results may differ from the reference program's by a relative error of at most 0.001.
Values are sent between devices in bfloat16 or wider.
A program may use at most 768 MiB of HBM per device.

```python
import jax
import jax.numpy as jnp

ROWS_DEV = 256
GROUPS = 256
PROTOS = 1024
EMBED_DIM = 256
SINK_ITERS = 3
SINK_EPS = 0.05
SOFT_TEMP = 0.1


def unit_rows(matrix):
    return matrix / jnp.sqrt(jnp.sum(matrix * matrix, axis=1, keepdims=True))


def draw_mask(draw_key):
    count_key, order_key = jax.random.split(draw_key)
    counts = jax.random.randint(count_key, (GROUPS,), 1, ROWS_DEV + 1)
    counts = counts.at[0].set(ROWS_DEV).at[1].set(1)
    order_scores = jax.random.randint(order_key, (GROUPS, ROWS_DEV), 0, 1 << 20) * ROWS_DEV + jnp.arange(ROWS_DEV, dtype=jnp.int32)[None, :]
    row_ranks = jnp.argsort(jnp.argsort(order_scores, axis=1), axis=1)
    return (row_ranks < counts[:, None]).astype(jnp.int32).reshape(-1)


def draw_picks(draw_key):
    band_width = max(2 * PROTOS // GROUPS, 1)
    starts = jnp.arange(GROUPS, dtype=jnp.int32)[:, None] * (PROTOS // GROUPS)
    offsets = jax.random.randint(draw_key, (GROUPS, ROWS_DEV), 0, band_width)
    return ((starts + offsets) % PROTOS).reshape(-1)


def draw_view(draw_key, protos, pick_ids):
    noise_rows = jax.random.normal(draw_key, (GROUPS * ROWS_DEV, EMBED_DIM), jnp.float32) * EMBED_DIM ** -0.5
    return unit_rows(0.6 * protos[pick_ids] + 0.8 * noise_rows)


def setup_inputs(seed: int = 0) -> dict:
    root_key = jax.random.key(seed)
    proto_key, pick_key, one_key, two_key, mask_key = jax.random.split(root_key, 5)
    protos = unit_rows(jax.random.normal(proto_key, (PROTOS, EMBED_DIM), jnp.float32))
    pick_ids = draw_picks(pick_key)
    return {
        "view_one": draw_view(one_key, protos, pick_ids).astype(jnp.bfloat16),
        "view_two": draw_view(two_key, protos, pick_ids).astype(jnp.bfloat16),
        "protos": protos.astype(jnp.bfloat16),
        "valid_mask": draw_mask(mask_key),
    }


def sinkhorn_codes(scores, weights, valid_count):
    transport = jnp.exp(scores / SINK_EPS) * weights
    for sweep_idx in range(SINK_ITERS):
        col_sum = jnp.sum(transport, axis=0, keepdims=True)
        transport = transport / (PROTOS * col_sum)
        row_sum = jnp.sum(transport, axis=1, keepdims=True) + (1.0 - weights)
        transport = transport / (valid_count * row_sum)
    return transport * valid_count


def reference(view_one, view_two, protos, valid_mask):
    weights = valid_mask.astype(jnp.float32)[:, None]
    valid_count = jnp.sum(weights)
    score_one = jnp.dot(view_one, protos.T, preferred_element_type=jnp.float32)
    score_two = jnp.dot(view_two, protos.T, preferred_element_type=jnp.float32)
    codes_one = sinkhorn_codes(score_one, weights, valid_count)
    codes_two = sinkhorn_codes(score_two, weights, valid_count)
    logp_one = jax.nn.log_softmax(score_one / SOFT_TEMP, axis=1)
    logp_two = jax.nn.log_softmax(score_two / SOFT_TEMP, axis=1)
    loss_value = -(jnp.sum(codes_two * logp_one) + jnp.sum(codes_one * logp_two)) / (2.0 * valid_count)
    grad_scale = weights / (2.0 * valid_count * SOFT_TEMP)
    grad_one = ((jnp.exp(logp_one) - codes_two) * grad_scale).astype(jnp.bfloat16)
    grad_two = ((jnp.exp(logp_two) - codes_one) * grad_scale).astype(jnp.bfloat16)
    dz_one = jnp.dot(grad_one, protos, preferred_element_type=jnp.float32)
    dz_two = jnp.dot(grad_two, protos, preferred_element_type=jnp.float32)
    d_protos = (jnp.dot(grad_one.T, view_one, preferred_element_type=jnp.float32)
                + jnp.dot(grad_two.T, view_two, preferred_element_type=jnp.float32))
    return codes_one, codes_two, loss_value, dz_one, dz_two, d_protos
```

```python
import functools

import jax
import jax.numpy as jnp
from jax import lax
from jax.experimental import pallas as pl
from jax.experimental.pallas import tpu as pltpu
from jax.sharding import PartitionSpec as P

MESH = pl.DeviceIdType.MESH
F32 = jnp.float32
BF16 = jnp.bfloat16
INV_TEMP = 10.0
LANES = 128


def torus(devices):
    return {256: (4, 4, 8), 16: (2, 2, 2)}[devices]


class Place:
    def __init__(self, dims):
        nx, ny, nz = dims
        self.np, self.nz = nx * ny, nz
        me = lax.axis_index("data")
        self.core = lax.rem(me, 2)
        self.p = lax.rem(me // 2, self.np)
        self.z = me // (2 * self.np)
        x, y = lax.rem(self.p, nx), self.p // nx

        def ring(d, n):
            return min(d, n - d)

        steps = [(dx, dy) for dy in range(ny) for dx in range(nx) if dx or dy]
        steps.sort(key=lambda s: -(ring(s[0], nx) + ring(s[1], ny)))
        self.plane_p = [lax.rem(y + dy, ny) * nx + lax.rem(x + dx, nx) for dx, dy in steps]
        self.plane = [self.at(self.z, p, self.core) for p in self.plane_p]
        dzs = sorted(range(1, nz), key=lambda d: -ring(d, nz))
        self.column_z = [lax.rem(self.z + d, nz) for d in dzs]
        self.column = [self.at(z, self.p, self.core) for z in self.column_z]
        self.column_other = [self.at(z, self.p, 1 - self.core) for z in self.column_z]
        self.partner = self.at(self.z, self.p, 1 - self.core)

    def at(self, z, p, core):
        return (z * self.np + p) * 2 + core

    def far_first(self, j):
        half = self.nz // 2
        d = jnp.where(lax.rem(j, 2) == 1, half - (j + 1) // 2, half + j // 2)
        return lax.rem(self.z + d, self.nz)


def send(src, dst, send_sem, recv_sem, device):
    copy = pltpu.make_async_remote_copy(
        src_ref=src, dst_ref=dst, send_sem=send_sem, recv_sem=recv_sem, device_id=(device,), device_id_type=MESH
    )
    copy.start()
    return copy


def wait_bytes(ref, sem):
    pltpu.make_async_copy(ref, ref, sem).wait()


def enter(devices):
    barrier = pltpu.get_barrier_semaphore()
    for device in devices:
        pl.semaphore_signal(barrier, inc=1, device_id=(device,), device_id_type=MESH)


def entered(devices):
    pl.semaphore_wait(pltpu.get_barrier_semaphore(), len(devices))


def column_of(row):
    return jnp.transpose(jnp.broadcast_to(row, (LANES, LANES)))[:, :1]


def sinkhorn_kernel(dims, z1_ref, z2_ref, c_ref, m_ref, out_ref, zs, ms, mcol, plan, xyb, zb, zlast,
                    pair_send, pair_recv, xy_send, xy_recv, z_send, z_recv):
    here = Place(dims)
    rows, protos = z1_ref.shape[0], c_ref.shape[0]
    groups = here.plane + here.column + here.column_other + [here.partner]
    enter(groups)
    first = here.core == 0

    zs[0:rows, :] = jnp.where(first, z1_ref[...], z2_ref[...])
    for h in range(rows // LANES):
        mcol[h * LANES:(h + 1) * LANES, :] = column_of(m_ref[h:h + 1, :].astype(F32))

    def fill(i, acc):
        at = pl.ds(pl.multiple_of(i * LANES, LANES), LANES)
        s = lax.dot_general(zs[at, :], c_ref[...], (((1,), (1,)), ((), ())), preferred_element_type=F32)
        e = jnp.exp(s * INV_TEMP)
        e = e * e
        plan[at, :] = e
        return acc + jnp.sum((e * mcol[at, :]).reshape(LANES // 8, 8, protos), axis=0)

    acc = lax.fori_loop(0, rows // LANES, fill, jnp.zeros((8, protos), F32))

    entered(groups)

    @pl.when(first)
    def _():
        send(z2_ref, zs.at[pl.ds(rows, rows)], pair_send.at[0], pair_recv.at[0], here.partner)

    @pl.when(jnp.logical_not(first))
    def _():
        send(z1_ref, zs.at[pl.ds(rows, rows)], pair_send.at[0], pair_recv.at[0], here.partner)

    mask_copy = send(m_ref, ms, pair_send.at[1], pair_recv.at[1], here.partner)
    mask_copy.wait()
    for h in range(rows // LANES):
        mcol[rows + h * LANES:rows + (h + 1) * LANES, :] = column_of(ms[h:h + 1, :].astype(F32))
    count = jnp.sum((m_ref[...] + ms[...]).astype(F32), keepdims=True)
    wait_bytes(zs.at[pl.ds(rows, rows)], pair_recv.at[0])
    wait_bytes(zs.at[pl.ds(0, rows)], pair_send.at[0])
    acc = lax.fori_loop(rows // LANES, 2 * rows // LANES, fill, acc)

    def chunk_sum(acc):
        return jnp.sum(acc, axis=0, keepdims=True)

    sent = []

    def all_sum(t, value, last):
        xyb[t, here.p] = jnp.concatenate([value, jnp.broadcast_to(count, (1, LANES))], axis=1)
        mine = xyb.at[t, here.p]
        for i, device in enumerate(here.plane):
            sent.append(send(mine, mine, xy_send.at[t, i], xy_recv.at[t], device))
        wait_bytes(xyb.at[t, pl.ds(0, here.np - 1)], xy_recv.at[t])
        part = jnp.sum(xyb[t], axis=0)
        if not last:
            zb[t, here.z] = part
            mine = zb.at[t, here.z]
            for i, device in enumerate(here.column):
                sent.append(send(mine, mine, z_send.at[t, i], z_recv.at[t], device))
            wait_bytes(zb.at[t, pl.ds(0, here.nz - 1)], z_recv.at[t])
            return jnp.sum(zb[t], axis=0)[:, :protos]
        slot = here.core * here.nz + here.z
        zlast[slot] = part
        mine = zlast.at[slot]
        targets = here.column + here.column_other + [here.partner]
        for i, device in enumerate(targets):
            sent.append(send(mine, mine, z_send.at[t, i], z_recv.at[t], device))
        wait_bytes(zlast.at[pl.ds(0, 2 * here.nz - 1)], z_recv.at[t])
        for view in range(2):
            out_ref[view] = jnp.sum(zlast[view * here.nz:(view + 1) * here.nz], axis=0)
        return None

    def sweep(a):
        step = 32

        def body(i, acc):
            at = pl.ds(pl.multiple_of(i * step, step), step)
            e = plan[at, :]
            m = mcol[at, :]
            r = jnp.sum(e * a, axis=1, keepdims=True) * m + (1.0 - m)
            return acc + jnp.sum((e * (m / r)).reshape(step // 8, 8, protos), axis=0)

        return lax.fori_loop(0, 2 * rows // step, body, jnp.zeros((8, protos), F32), unroll=2)

    for t in range(3):
        total = all_sum(t, chunk_sum(acc), t == 2)
        if t < 2:
            acc = sweep(1.0 / (protos * total))
    for copy in sent:
        copy.wait_send()


def sinkhorn_columns(dims, view_one, view_two, protos, mask):
    rows, depth = view_one.shape
    count = protos.shape[0]
    width = count + LANES
    n_plane, n_z = dims[0] * dims[1], dims[2]
    vmem = pl.BlockSpec(memory_space=pltpu.VMEM)
    return pl.pallas_call(
        functools.partial(sinkhorn_kernel, dims),
        out_shape=jax.ShapeDtypeStruct((2, 1, width), F32),
        in_specs=[vmem] * 4,
        out_specs=vmem,
        scratch_shapes=[
            pltpu.VMEM((2 * rows, depth), BF16),
            pltpu.VMEM((rows // LANES, LANES), jnp.int32),
            pltpu.VMEM((2 * rows, 1), F32),
            pltpu.VMEM((2 * rows, count), F32),
            pltpu.VMEM((3, n_plane, 1, width), F32),
            pltpu.VMEM((2, n_z, 1, width), F32),
            pltpu.VMEM((2 * n_z, 1, width), F32),
            pltpu.SemaphoreType.DMA((2,)),
            pltpu.SemaphoreType.DMA((2,)),
            pltpu.SemaphoreType.DMA((3, n_plane - 1)),
            pltpu.SemaphoreType.DMA((3,)),
            pltpu.SemaphoreType.DMA((3, 2 * n_z - 1)),
            pltpu.SemaphoreType.DMA((3,)),
        ],
        compiler_params=pltpu.CompilerParams(collective_id=0, has_side_effects=True),
        name="sinkhorn",
    )(view_one, view_two, protos, mask.reshape(rows // LANES, LANES))


def reduce_kernel(dims, part_ref, loss_ref, out_ref, loss_out, part, inbox, half, rs, tot, zrs, full,
                  lpair, lxy, lz, c_send, c_recv, r_send, r_recv, t_send, t_recv,
                  g_send, g_recv, x_send, x_recv, d_send, d_recv, l_send, l_recv):
    here = Place(dims)
    n_plane, n_z = here.np, here.nz
    chunk = part.shape[3]
    groups = here.plane + here.column + [here.partner]
    enter(groups)
    for h in range(2):
        part[h] = part_ref[:, h * LANES:(h + 1) * LANES].reshape(n_z, n_plane, chunk, LANES)
    lpair[here.core] = loss_ref[...]
    entered(groups)

    sent = []
    lmine = lpair.at[here.core]
    sent.append(send(lmine, lmine, l_send.at[0], l_recv.at[0], here.partner))

    other = 1 - here.core

    def give(j, _):
        z = here.far_first(j)
        send(part.at[other, z], inbox.at[z], c_send.at[j], c_recv.at[j], here.partner)
        return 0

    lax.fori_loop(0, n_z, give, 0)

    def spread(j, _):
        z = here.far_first(j)
        wait_bytes(inbox.at[z], c_recv.at[j])
        half[z] = part[here.core, z] + inbox[z]
        rs[here.p, z] = half[z, here.p]
        for i in range(n_plane - 1):
            send(half.at[z, here.plane_p[i]], rs.at[here.p, z], r_send.at[j, i], r_recv.at[j], here.plane[i])
        return 0

    lax.fori_loop(0, n_z, spread, 0)

    wait_bytes(lpair.at[0], l_recv.at[0])
    lxy[here.p] = lpair[0] + lpair[1]
    lmine = lxy.at[here.p]
    for i, device in enumerate(here.plane):
        sent.append(send(lmine, lmine, l_send.at[1 + i], l_recv.at[1], device))

    def gather(j, _):
        z = here.far_first(j)
        wait_bytes(rs.at[pl.ds(0, n_plane - 1), z], r_recv.at[j])
        tot[z] = jnp.sum(rs[:, z], axis=0)

        @pl.when(j < n_z - 1)
        def _():
            send(tot.at[z], zrs.at[here.z], t_send.at[j], t_recv.at[0], here.at(z, here.p, here.core))

        return 0

    lax.fori_loop(0, n_z, gather, 0)
    wait_bytes(lxy.at[pl.ds(0, n_plane - 1)], l_recv.at[1])
    lz[here.z] = jnp.sum(lxy[...], axis=0)
    lmine = lz.at[here.z]
    for i, device in enumerate(here.column):
        sent.append(send(lmine, lmine, l_send.at[n_plane + i], l_recv.at[2], device))

    zrs[here.z] = tot[here.z]
    wait_bytes(zrs.at[pl.ds(0, n_z - 1)], t_recv.at[0])
    full[here.core, here.z, here.p] = jnp.sum(zrs[...], axis=0)

    def near_first(j):
        return here.far_first(n_z - 1 - j)

    mine = full.at[here.core, here.z, here.p]
    for i, device in enumerate(here.column):
        sent.append(send(mine, mine, g_send.at[i], g_recv.at[here.z], device))

    def forward(j, _):
        z = near_first(j)
        held = full.at[here.core, z, here.p]

        @pl.when(j > 0)
        def _():
            wait_bytes(held, g_recv.at[z])

        for i in range(n_plane - 1):
            send(held, held, x_send.at[j, i], x_recv.at[j], here.plane[i])
        return 0

    lax.fori_loop(0, n_z, forward, 0)

    def cross(j, _):
        z = near_first(j)
        wait_bytes(full.at[here.core, z, pl.ds(0, n_plane - 1)], x_recv.at[j])
        held = full.at[here.core, z]
        send(held, held, d_send.at[j], d_recv.at[j], here.partner)
        return 0

    lax.fori_loop(0, n_z, cross, 0)

    wait_bytes(lz.at[pl.ds(0, n_z - 1)], l_recv.at[2])
    loss_out[...] = jnp.sum(lz[...], axis=0)

    def finish(j, _):
        z = near_first(j)
        wait_bytes(full.at[other, z], d_recv.at[j])
        wait_bytes(full.at[here.core, z], d_send.at[j])
        wait_bytes(inbox.at[z], c_send.at[j])

        @pl.when(j < n_z - 1)
        def _():
            wait_bytes(tot.at[z], t_send.at[j])

        for i in range(n_plane - 1):
            wait_bytes(tot.at[z], r_send.at[j, i])
            wait_bytes(tot.at[z], x_send.at[j, i])
        return 0

    lax.fori_loop(0, n_z, finish, 0)
    for h in range(2):
        out_ref[:, h * LANES:(h + 1) * LANES] = full[h].reshape(n_z * n_plane * chunk, LANES)
    for copy in sent:
        copy.wait_send()


def reduce_all(dims, part, loss_row):
    count, depth = part.shape
    n_plane, n_z = dims[0] * dims[1], dims[2]
    chunk = count // (n_plane * n_z)
    vmem = pl.BlockSpec(memory_space=pltpu.VMEM)
    dma = pltpu.SemaphoreType.DMA
    return pl.pallas_call(
        functools.partial(reduce_kernel, dims),
        out_shape=(jax.ShapeDtypeStruct((count, depth), F32), jax.ShapeDtypeStruct((1, LANES), F32)),
        in_specs=[vmem] * 2,
        out_specs=(vmem, vmem),
        scratch_shapes=[
            pltpu.VMEM((2, n_z, n_plane, chunk, LANES), F32),
            pltpu.VMEM((n_z, n_plane, chunk, LANES), F32),
            pltpu.VMEM((n_z, n_plane, chunk, LANES), F32),
            pltpu.VMEM((n_plane, n_z, chunk, LANES), F32),
            pltpu.VMEM((n_z, chunk, LANES), F32),
            pltpu.VMEM((n_z, chunk, LANES), F32),
            pltpu.VMEM((2, n_z, n_plane, chunk, LANES), F32),
            pltpu.VMEM((2, 1, LANES), F32),
            pltpu.VMEM((n_plane, 1, LANES), F32),
            pltpu.VMEM((n_z, 1, LANES), F32),
            dma((n_z,)), dma((n_z,)),
            dma((n_z, n_plane - 1)), dma((n_z,)),
            dma((n_z,)), dma((1,)),
            dma((n_z - 1,)), dma((n_z,)),
            dma((n_z, n_plane - 1)), dma((n_z,)),
            dma((n_z,)), dma((n_z,)),
            dma((n_plane + n_z,)), dma((3,)),
        ],
        compiler_params=pltpu.CompilerParams(collective_id=1, has_side_effects=True),
        name="reduce_all",
    )(part, loss_row)


def solution(mesh):
    dims = torus(mesh.size)

    def local_step(view_one, view_two, protos, valid_mask):
        sums = sinkhorn_columns(dims, view_one, view_two, protos, valid_mask)
        count = protos.shape[0]
        valid_count = sums[0, 0, count]
        weights = valid_mask.astype(F32)[:, None]

        def scores(view):
            return jnp.einsum("nd,kd->nk", view, protos, preferred_element_type=F32) * INV_TEMP

        def codes(score, v):
            e = jnp.exp(score)
            a = 1.0 / (count * sums[v, :, :count])
            plan = e * e * a
            return plan * (weights / (weights * jnp.sum(plan, axis=1, keepdims=True) + (1.0 - weights)))

        s1, s2 = scores(view_one), scores(view_two)
        q1, q2 = codes(s1, 0), codes(s2, 1)
        logp1 = s1 - jnp.log(jnp.sum(jnp.exp(s1), axis=1, keepdims=True))
        logp2 = s2 - jnp.log(jnp.sum(jnp.exp(s2), axis=1, keepdims=True))
        part_loss = -(jnp.sum(q2 * logp1) + jnp.sum(q1 * logp2)) / (2.0 * valid_count)
        scale = weights * (0.5 * INV_TEMP) / valid_count
        g1 = ((jnp.exp(logp1) - q2) * scale).astype(BF16)
        g2 = ((jnp.exp(logp2) - q1) * scale).astype(BF16)
        dz1 = jnp.dot(g1, protos, preferred_element_type=F32)
        dz2 = jnp.dot(g2, protos, preferred_element_type=F32)
        part = (jnp.einsum("nk,nd->kd", g1, view_one, preferred_element_type=F32)
                + jnp.einsum("nk,nd->kd", g2, view_two, preferred_element_type=F32))
        d_protos, loss_row = reduce_all(dims, part, jnp.broadcast_to(part_loss, (1, LANES)))
        return q1, q2, loss_row[0, 0], dz1, dz2, d_protos

    return jax.shard_map(
        local_step,
        mesh=mesh,
        in_specs=(P("data", None), P("data", None), P(None, None), P("data")),
        out_specs=(P("data", None), P("data", None), P(), P("data", None), P("data", None), P(None, None)),
        check_vma=False,
    )
```

```python
import functools

import jax
import jax.numpy as jnp
from jax import lax
from jax.experimental import pallas as pl
from jax.experimental.pallas import tpu as pltpu
from jax.sharding import PartitionSpec as P

MESH = pl.DeviceIdType.MESH
F32 = jnp.float32
BF16 = jnp.bfloat16
INV_TEMP = 10.0
LANES = 128


def torus(devices):
    return {256: (4, 4, 8), 16: (2, 2, 2)}[devices]


class Place:
    def __init__(self, dims):
        nx, ny, nz = dims
        self.np, self.nz = nx * ny, nz
        me = lax.axis_index("data")
        self.core = lax.rem(me, 2)
        self.p = lax.rem(me // 2, self.np)
        self.z = me // (2 * self.np)
        x, y = lax.rem(self.p, nx), self.p // nx

        def ring(d, n):
            return min(d, n - d)

        steps = [(dx, dy) for dy in range(ny) for dx in range(nx) if dx or dy]
        steps.sort(key=lambda s: -(ring(s[0], nx) + ring(s[1], ny)))
        self.plane_p = [lax.rem(y + dy, ny) * nx + lax.rem(x + dx, nx) for dx, dy in steps]
        self.plane = [self.at(self.z, p, self.core) for p in self.plane_p]
        dzs = sorted(range(1, nz), key=lambda d: -ring(d, nz))
        self.column_z = [lax.rem(self.z + d, nz) for d in dzs]
        self.column = [self.at(z, self.p, self.core) for z in self.column_z]
        self.column_other = [self.at(z, self.p, 1 - self.core) for z in self.column_z]
        self.partner = self.at(self.z, self.p, 1 - self.core)

    def at(self, z, p, core):
        return (z * self.np + p) * 2 + core

    def far_first(self, j):
        half = self.nz // 2
        d = jnp.where(lax.rem(j, 2) == 1, half - (j + 1) // 2, half + j // 2)
        return lax.rem(self.z + d, self.nz)


def send(src, dst, send_sem, recv_sem, device):
    copy = pltpu.make_async_remote_copy(
        src_ref=src, dst_ref=dst, send_sem=send_sem, recv_sem=recv_sem, device_id=(device,), device_id_type=MESH
    )
    copy.start()
    return copy


def wait_bytes(ref, sem):
    pltpu.make_async_copy(ref, ref, sem).wait()


def enter(devices):
    barrier = pltpu.get_barrier_semaphore()
    for device in devices:
        pl.semaphore_signal(barrier, inc=1, device_id=(device,), device_id_type=MESH)


def entered(devices):
    pl.semaphore_wait(pltpu.get_barrier_semaphore(), len(devices))


def column_of(row):
    return jnp.transpose(jnp.broadcast_to(row, (LANES, LANES)))[:, :1]


def step_kernel(dims, z1_hbm, z2_hbm, c_hbm, m_hbm, q_out, dz_out, dc_out, loss_out,
                zin, cbuf, zx, m_own, ms, mcol, bcol, avec, plan, plan_other, prob, logp, grad, zt,
                xy_first, spare, xyb, z_first, zb, zlast, part, inbox, half, rs, tot, zrs, full, flip, lpair, lxy, lz,
                in_sem, pair_send, pair_recv, f_send, f_recv, xy_send, xy_recv, z_send, z_recv,
                c_send, c_recv, r_send, r_recv, t_send, t_recv,
                g_send, g_recv, x_send, x_recv, d_send, d_recv, l_send, l_recv):
    here = Place(dims)
    n_plane, n_z = here.np, here.nz
    rows, protos = zin.shape[1], cbuf.shape[0]
    block = protos // n_z
    mine, other = here.core, 1 - here.core
    plane_other = [here.at(here.z, p, other) for p in here.plane_p]
    groups = here.plane + plane_other + here.column + here.column_other + [here.partner]
    enter(groups)

    loads = [pltpu.make_async_copy(z1_hbm, zin.at[0], in_sem.at[0]),
             pltpu.make_async_copy(z2_hbm, zin.at[1], in_sem.at[1]),
             pltpu.make_async_copy(c_hbm, cbuf, in_sem.at[2]),
             pltpu.make_async_copy(m_hbm, m_own, in_sem.at[3])]
    for load in loads:
        load.start()
    loads[3].wait()
    mask = m_own[...].astype(F32)
    for h in range(rows // LANES):
        mcol[h * LANES:(h + 1) * LANES, :] = column_of(mask[h:h + 1, :])
    count = jnp.broadcast_to(jnp.sum(mask, keepdims=True), (1, LANES))
    for load in loads[:3]:
        load.wait()

    def scores(z):
        return lax.dot_general(z, cbuf[...], (((1,), (1,)), ((), ())), preferred_element_type=F32) * INV_TEMP

    def fold(e, m):
        return jnp.sum((e * m).reshape(LANES // 8, 8, protos), axis=0)

    def fill(i, accs):
        at = pl.ds(pl.multiple_of(i * LANES, LANES), LANES)
        out = []
        for view, plan_ref, acc in ((mine, plan, accs[0]), (other, plan_other, accs[1])):
            s = scores(zin[view, at, :])
            logp[view, at, :] = s
            e = jnp.exp(s)
            e = e * e
            plan_ref[at, :] = e
            out.append(acc + fold(e, mcol[at, :]))
        return tuple(out)

    zero = jnp.zeros((8, protos), F32)
    acc_mine, acc_other = lax.fori_loop(0, rows // LANES, fill, (zero, zero))

    def payload(acc):
        return jnp.concatenate([jnp.sum(acc, axis=0, keepdims=True), count], axis=1)

    sent = []
    slot = here.core * n_plane + here.p
    xy_first[slot] = payload(acc_mine)
    spare[...] = payload(acc_other)

    entered(groups)

    held = xy_first.at[slot]
    for i in range(n_plane - 1):
        sent.append(send(held, held, f_send.at[i], f_recv.at[0], here.plane[i]))
        sent.append(send(spare, held, f_send.at[n_plane + i], f_recv.at[0], plane_other[i]))
    sent.append(send(spare, held, f_send.at[n_plane - 1], f_recv.at[0], here.partner))
    sent.append(send(zin.at[other], zx, pair_send.at[0], pair_recv.at[0], here.partner))
    sent.append(send(m_own, ms, pair_send.at[1], pair_recv.at[1], here.partner))

    wait_bytes(ms, pair_recv.at[1])
    for h in range(rows // LANES):
        mcol[rows + h * LANES:rows + (h + 1) * LANES, :] = column_of(ms[h:h + 1, :].astype(F32))
    wait_bytes(zx, pair_recv.at[0])

    def fill_partner(i, _):
        e = jnp.exp(scores(zx[pl.ds(pl.multiple_of(i * LANES, LANES), LANES), :]))
        plan[pl.ds(pl.multiple_of(rows + i * LANES, LANES), LANES), :] = e * e
        return 0

    lax.fori_loop(0, rows // LANES, fill_partner, 0)

    def to_column(t, value, last):
        if not last:
            held = (z_first if t == 0 else zb).at[here.z]
            held[...] = value
            for i, device in enumerate(here.column):
                sent.append(send(held, held, z_send.at[t, i], z_recv.at[t], device))
            return
        slot = here.core * n_z + here.z
        zlast[slot] = value
        held = zlast.at[slot]
        for i, device in enumerate(here.column + here.column_other + [here.partner]):
            sent.append(send(held, held, z_send.at[t, i], z_recv.at[t], device))

    def from_column(t):
        buf = z_first if t == 0 else zb
        wait_bytes(buf.at[pl.ds(0, n_z - 1)], z_recv.at[t])
        return jnp.sum(buf[...], axis=0)

    def to_plane(t, value):
        xyb[t, here.p] = value
        held = xyb.at[t, here.p]
        for i, device in enumerate(here.plane):
            sent.append(send(held, held, xy_send.at[t, i], xy_recv.at[t], device))

    def from_plane(t):
        wait_bytes(xyb.at[t, pl.ds(0, n_plane - 1)], xy_recv.at[t])
        return jnp.sum(xyb[t], axis=0)

    def sweep(a):
        step = 32

        def body(i, acc):
            at = pl.ds(pl.multiple_of(i * step, step), step)
            e = plan[at, :]
            m = mcol[at, :]
            r = jnp.sum(e * a, axis=1, keepdims=True) * m + (1.0 - m)
            return acc + jnp.sum((e * (m / r)).reshape(step // 8, 8, protos), axis=0)

        acc = lax.fori_loop(0, 2 * rows // step, body, zero, unroll=2)
        return jnp.sum(acc, axis=0, keepdims=True)

    wait_bytes(xy_first.at[pl.ds(0, 2 * n_plane - 1)], f_recv.at[0])
    to_column(0, jnp.sum(xy_first[...], axis=0), False)

    def soften(i, _):
        at = pl.ds(pl.multiple_of(i * 32, 32), 32)
        for view in range(2):
            s = logp[view, at, :]
            s = s - jnp.log(jnp.sum(jnp.exp(s), axis=1, keepdims=True))
            logp[view, at, :] = s
            prob[view, at, :] = jnp.exp(s)
        return 0

    lax.fori_loop(0, rows // 32, soften, 0)
    for k, view in enumerate((mine, other)):
        zt[:, k * rows:(k + 1) * rows] = jnp.transpose(zin[view].astype(F32)).astype(BF16)

    total = from_column(0)
    valid = total[:, protos:]
    for t in (0, 1):
        a = 1.0 / (protos * total[:, :protos])
        to_plane(t, sweep(a))
        if t == 0:
            to_column(1, from_plane(0), False)
            total = from_column(1)
        else:
            to_column(2, from_plane(1), True)
    wait_bytes(zlast.at[pl.ds(0, 2 * n_z - 1)], z_recv.at[2])
    for view in range(2):
        avec[view] = 1.0 / (protos * jnp.sum(zlast[view * n_z:(view + 1) * n_z], axis=0))

    def weigh(i, _):
        at = pl.ds(pl.multiple_of(i * 32, 32), 32)
        m = mcol[at, :]
        for k, (view, plan_ref) in enumerate(((mine, plan), (other, plan_other))):
            r = jnp.sum(plan_ref[at, :] * avec[view], axis=1, keepdims=True) * m + (1.0 - m)
            bcol[k, at, :] = m / r
        return 0

    lax.fori_loop(0, rows // 32, weigh, 0)
    scale = mcol[0:rows, :] * (0.5 * INV_TEMP) / valid[:, :1]

    def derive(j, _):
        z = here.far_first(j)
        cols = pl.ds(pl.multiple_of(z * block, block), block)
        q_mine = plan[0:rows, cols] * avec[mine, :, cols] * bcol[0]
        q_other = plan_other[:, cols] * avec[other, :, cols] * bcol[1]
        q_out[mine, :, cols] = q_mine
        q_out[other, :, cols] = q_other
        g = jnp.concatenate([((prob[mine, :, cols] - q_other) * scale).astype(BF16),
                             ((prob[other, :, cols] - q_mine) * scale).astype(BF16)], axis=0)
        grad[:, cols] = g
        d = lax.dot_general(zt[...], g, (((1,), (0,)), ((), ())), preferred_element_type=F32)
        part[z] = d.reshape(part.shape[1:])
        send(part.at[z, other], inbox.at[z], c_send.at[j], c_recv.at[j], here.partner)
        return 0

    lax.fori_loop(0, n_z, derive, 0)

    def spread(j, _):
        z = here.far_first(j)
        wait_bytes(inbox.at[z], c_recv.at[j])
        half[z] = part[z, mine] + inbox[z]
        rs[here.p, z] = half[z, here.p]
        for i in range(n_plane - 1):
            send(half.at[z, here.plane_p[i]], rs.at[here.p, z], r_send.at[j, i], r_recv.at[j], here.plane[i])
        return 0

    lax.fori_loop(0, n_z, spread, 0)

    def lose(i, acc):
        at = pl.ds(pl.multiple_of(i * 32, 32), 32)
        pair = q_out[1, at, :] * logp[0, at, :] + q_out[0, at, :] * logp[1, at, :]
        return acc + jnp.sum(pair.reshape(4, 8, protos), axis=0)

    loss = jnp.sum(lax.fori_loop(0, rows // 32, lose, zero), keepdims=True)
    lpair[here.core] = jnp.broadcast_to(loss, (1, LANES)) * (-0.5) / valid
    lheld = lpair.at[here.core]
    sent.append(send(lheld, lheld, l_send.at[0], l_recv.at[0], here.partner))

    def descend(i, _):
        at = pl.ds(pl.multiple_of(i * LANES, LANES), LANES)
        for k, view in enumerate((mine, other)):
            g = grad[pl.ds(pl.multiple_of(k * rows + i * LANES, LANES), LANES), :]
            dz_out[view, at, :] = jnp.dot(g, cbuf[...], preferred_element_type=F32)
        return 0

    lax.fori_loop(0, rows // LANES, descend, 0)

    wait_bytes(lpair.at[0], l_recv.at[0])
    lxy[here.p] = lpair[0] + lpair[1]
    lheld = lxy.at[here.p]
    for i, device in enumerate(here.plane):
        sent.append(send(lheld, lheld, l_send.at[1 + i], l_recv.at[1], device))

    def gather(j, _):
        z = here.far_first(j)
        wait_bytes(rs.at[pl.ds(0, n_plane - 1), z], r_recv.at[j])
        tot[z] = jnp.sum(rs[:, z], axis=0)

        @pl.when(j < n_z - 1)
        def _():
            send(tot.at[z], zrs.at[here.z], t_send.at[j], t_recv.at[0], here.at(z, here.p, here.core))

        return 0

    lax.fori_loop(0, n_z, gather, 0)
    wait_bytes(lxy.at[pl.ds(0, n_plane - 1)], l_recv.at[1])
    lz[here.z] = jnp.sum(lxy[...], axis=0)
    lheld = lz.at[here.z]
    for i, device in enumerate(here.column):
        sent.append(send(lheld, lheld, l_send.at[n_plane + i], l_recv.at[2], device))

    zrs[here.z] = tot[here.z]
    wait_bytes(zrs.at[pl.ds(0, n_z - 1)], t_recv.at[0])
    full[here.z, here.p] = jnp.sum(zrs[...], axis=0)

    def near_first(j):
        return here.far_first(n_z - 1 - j)

    held = full.at[here.z, here.p]
    for i, device in enumerate(here.column):
        sent.append(send(held, held, g_send.at[i], g_recv.at[here.z], device))

    def forward(j, _):
        z = near_first(j)
        held = full.at[z, here.p]

        @pl.when(j > 0)
        def _():
            wait_bytes(held, g_recv.at[z])

        for i in range(n_plane - 1):
            send(held, held, x_send.at[j, i], x_recv.at[j], here.plane[i])
        return 0

    lax.fori_loop(0, n_z, forward, 0)

    def put(z, which):
        at = pl.ds(pl.multiple_of(z * block, block), block)
        dc_out[at, pl.ds(pl.multiple_of(which * LANES, LANES), LANES)] = flip[which, z]

    def cross(j, _):
        z = near_first(j)
        wait_bytes(full.at[z, pl.ds(0, n_plane - 1)], x_recv.at[j])
        flip[mine, z] = jnp.transpose(full[z].reshape(LANES, block))
        held = flip.at[mine, z]
        send(held, held, d_send.at[j], d_recv.at[j], here.partner)
        put(z, mine)
        return 0

    lax.fori_loop(0, n_z, cross, 0)

    wait_bytes(lz.at[pl.ds(0, n_z - 1)], l_recv.at[2])
    loss_out[...] = jnp.sum(lz[...], axis=0)

    def finish(j, _):
        z = near_first(j)
        wait_bytes(flip.at[other, z], d_recv.at[j])
        put(z, other)
        wait_bytes(flip.at[mine, z], d_send.at[j])
        wait_bytes(inbox.at[z], c_send.at[j])

        @pl.when(j < n_z - 1)
        def _():
            wait_bytes(tot.at[z], t_send.at[j])

        for i in range(n_plane - 1):
            wait_bytes(tot.at[z], r_send.at[j, i])
            wait_bytes(tot.at[z], x_send.at[j, i])
        return 0

    lax.fori_loop(0, n_z, finish, 0)
    for copy in sent:
        copy.wait_send()


def whole_step(dims, view_one, view_two, protos, mask):
    rows, depth = view_one.shape
    count = protos.shape[0]
    width = count + LANES
    n_plane, n_z = dims[0] * dims[1], dims[2]
    block = count // n_z
    tile = (LANES // n_plane, block)
    vmem = pl.BlockSpec(memory_space=pltpu.VMEM)
    hbm = pl.BlockSpec(memory_space=pltpu.HBM)
    dma, mem = pltpu.SemaphoreType.DMA, pltpu.VMEM
    return pl.pallas_call(
        functools.partial(step_kernel, dims),
        out_shape=(mem((2, rows, count), F32), mem((2, rows, depth), F32), mem((count, depth), F32), mem((1, LANES), F32)),
        in_specs=[hbm] * 4,
        out_specs=(vmem,) * 4,
        scratch_shapes=[
            mem((2, rows, depth), BF16),
            mem((count, depth), BF16),
            mem((rows, depth), BF16),
            mem((rows // LANES, LANES), jnp.int32),
            mem((rows // LANES, LANES), jnp.int32),
            mem((2 * rows, 1), F32),
            mem((2, rows, 1), F32),
            mem((2, 1, count), F32),
            mem((2 * rows, count), F32),
            mem((rows, count), F32),
            mem((2, rows, count), F32),
            mem((2, rows, count), F32),
            mem((2 * rows, count), BF16),
            mem((depth, 2 * rows), BF16),
            mem((2 * n_plane, 1, width), F32),
            mem((1, width), F32),
            mem((2, n_plane, 1, width - LANES), F32),
            mem((n_z, 1, width), F32),
            mem((n_z, 1, width - LANES), F32),
            mem((2 * n_z, 1, width - LANES), F32),
            mem((n_z, 2, n_plane) + tile, F32),
            mem((n_z, n_plane) + tile, F32),
            mem((n_z, n_plane) + tile, F32),
            mem((n_plane, n_z) + tile, F32),
            mem((n_z,) + tile, F32),
            mem((n_z,) + tile, F32),
            mem((n_z, n_plane) + tile, F32),
            mem((2, n_z, block, LANES), F32),
            mem((2, 1, LANES), F32),
            mem((n_plane, 1, LANES), F32),
            mem((n_z, 1, LANES), F32),
            dma((4,)),
            dma((2,)), dma((2,)),
            dma((2 * n_plane,)), dma((1,)),
            dma((2, n_plane - 1)), dma((2,)),
            dma((3, 2 * n_z - 1)), dma((3,)),
            dma((n_z,)), dma((n_z,)),
            dma((n_z, n_plane - 1)), dma((n_z,)),
            dma((n_z,)), dma((1,)),
            dma((n_z - 1,)), dma((n_z,)),
            dma((n_z, n_plane - 1)), dma((n_z,)),
            dma((n_z,)), dma((n_z,)),
            dma((n_plane + n_z,)), dma((3,)),
        ],
        compiler_params=pltpu.CompilerParams(collective_id=0, has_side_effects=True, vmem_limit_bytes=32 << 20),
        name="whole_step",
    )(*(pltpu.with_memory_space_constraint(x, pltpu.HBM)
        for x in (view_one, view_two, protos, mask.reshape(rows // LANES, LANES))))


def deliver_kernel(q_ref, dz_ref, dc_ref, loss_ref, q1, q2, dz1, dz2, dc, loss, sem):
    loss[...] = loss_ref[:, :1]
    moves = [(q_ref.at[0], q1), (q_ref.at[1], q2), (dz_ref.at[0], dz1), (dz_ref.at[1], dz2), (dc_ref, dc)]
    copies = [pltpu.make_async_copy(src, dst, sem.at[i]) for i, (src, dst) in enumerate(moves)]
    for copy in copies:
        copy.start()
    for copy in copies:
        copy.wait()


def deliver(q, dz, dc, loss):
    vmem = pl.BlockSpec(memory_space=pltpu.VMEM)
    hbm = pl.BlockSpec(memory_space=pltpu.HBM)
    shapes = [q.shape[1:]] * 2 + [dz.shape[1:]] * 2 + [dc.shape, (1, 1)]
    return pl.pallas_call(
        deliver_kernel,
        out_shape=[jax.ShapeDtypeStruct(shape, F32) for shape in shapes],
        in_specs=[vmem] * 4,
        out_specs=[hbm] * 5 + [vmem],
        scratch_shapes=[pltpu.SemaphoreType.DMA((5,))],
        compiler_params=pltpu.CompilerParams(vmem_limit_bytes=8 << 20),
        name="deliver",
    )(q, dz, dc, loss)


def solution(mesh):
    dims = torus(mesh.size)

    def local_step(view_one, view_two, protos, valid_mask):
        q, dz, dc, loss = whole_step(dims, view_one, view_two, protos, valid_mask)
        q1, q2, dz1, dz2, dc, loss = deliver(q, dz, dc, loss)
        return q1, q2, loss[0, 0], dz1, dz2, dc

    return jax.shard_map(
        local_step,
        mesh=mesh,
        in_specs=(P("data", None), P("data", None), P(None, None), P("data")),
        out_specs=(P("data", None), P("data", None), P(), P("data", None), P("data", None), P(None, None)),
        check_vma=False,
    )
```

```python
import functools

import jax
import jax.numpy as jnp
from jax import lax
from jax.experimental import pallas as pl
from jax.experimental.pallas import tpu as pltpu
from jax.sharding import PartitionSpec as P

MESH = pl.DeviceIdType.MESH
F32 = jnp.float32
BF16 = jnp.bfloat16
INV_TEMP = 10.0
LANES = 128


def torus(devices):
    return {256: (4, 4, 8), 16: (2, 2, 2)}[devices]


class Place:
    def __init__(self, dims):
        nx, ny, nz = dims
        self.np, self.nz = nx * ny, nz
        me = lax.axis_index("data")
        self.core = lax.rem(me, 2)
        self.p = lax.rem(me // 2, self.np)
        self.z = me // (2 * self.np)
        x, y = lax.rem(self.p, nx), self.p // nx

        def ring(d, n):
            return min(d, n - d)

        steps = [(dx, dy) for dy in range(ny) for dx in range(nx) if dx or dy]
        steps.sort(key=lambda s: -(ring(s[0], nx) + ring(s[1], ny)))
        self.plane_p = [lax.rem(y + dy, ny) * nx + lax.rem(x + dx, nx) for dx, dy in steps]
        self.plane = [self.at(self.z, p, self.core) for p in self.plane_p]
        dzs = sorted(range(1, nz), key=lambda d: -ring(d, nz))
        self.column_z = [lax.rem(self.z + d, nz) for d in dzs]
        self.column = [self.at(z, self.p, self.core) for z in self.column_z]
        self.partner = self.at(self.z, self.p, 1 - self.core)

    def at(self, z, p, core):
        return (z * self.np + p) * 2 + core

    def far_first(self, j):
        half = self.nz // 2
        d = jnp.where(lax.rem(j, 2) == 1, half - (j + 1) // 2, half + j // 2)
        return lax.rem(self.z + d, self.nz)


def send(src, dst, send_sem, recv_sem, device):
    copy = pltpu.make_async_remote_copy(
        src_ref=src, dst_ref=dst, send_sem=send_sem, recv_sem=recv_sem, device_id=(device,), device_id_type=MESH
    )
    copy.start()
    return copy


def wait_bytes(ref, sem):
    pltpu.make_async_copy(ref, ref, sem).wait()


def enter(devices):
    barrier = pltpu.get_barrier_semaphore()
    for device in devices:
        pl.semaphore_signal(barrier, inc=1, device_id=(device,), device_id_type=MESH)


def entered(devices):
    pl.semaphore_wait(pltpu.get_barrier_semaphore(), len(devices))


def column_of(row):
    return jnp.transpose(jnp.broadcast_to(row, (LANES, LANES)))[:, :1]


def step_kernel(dims, z1_hbm, z2_hbm, c_hbm, m_hbm, q_res, dz_res, dc_res, loss_out,
                q_out, dz_out, zin, cbuf, zx, m_own, ms, mcol, bcol, avec, plan, plan_other, prob, logp, grad, zt,
                xy_first, spare, xyb, z_first, zb, part, inbox, half, rs, tot, zrs, full, flip, lpair, lxy, lz,
                in_sem, out_sem, pair_send, pair_recv, f_send, f_recv, xy_send, xy_recv, z_send, z_recv,
                c_send, c_recv, r_send, r_recv, t_send, t_recv,
                g_send, g_recv, x_send, x_recv, d_send, d_recv, l_send, l_recv):
    here = Place(dims)
    n_plane, n_z = here.np, here.nz
    rows, protos = zin.shape[1], cbuf.shape[0]
    block = protos // n_z
    mine, other = here.core, 1 - here.core
    plane_other = [here.at(here.z, p, other) for p in here.plane_p]
    groups = here.plane + plane_other + here.column + [here.partner]
    enter(groups)

    loads = [pltpu.make_async_copy(z1_hbm, zin.at[0], in_sem.at[0]),
             pltpu.make_async_copy(z2_hbm, zin.at[1], in_sem.at[1]),
             pltpu.make_async_copy(c_hbm, cbuf, in_sem.at[2]),
             pltpu.make_async_copy(m_hbm, m_own, in_sem.at[3])]
    for load in loads:
        load.start()
    loads[3].wait()
    mask = m_own[...].astype(F32)
    for h in range(rows // LANES):
        mcol[h * LANES:(h + 1) * LANES, :] = column_of(mask[h:h + 1, :])
    count = jnp.broadcast_to(jnp.sum(mask, keepdims=True), (1, LANES))
    for load in loads[:3]:
        load.wait()

    def scores(z):
        return lax.dot_general(z, cbuf[...], (((1,), (1,)), ((), ())), preferred_element_type=F32) * INV_TEMP

    def fold(e, m):
        return jnp.sum((e * m).reshape(LANES // 8, 8, protos), axis=0)

    def fill(i, accs):
        at = pl.ds(pl.multiple_of(i * LANES, LANES), LANES)
        out = []
        for view, plan_ref, acc in ((mine, plan, accs[0]), (other, plan_other, accs[1])):
            s = scores(zin[view, at, :])
            logp[view, at, :] = s
            e = jnp.exp(s)
            e = e * e
            plan_ref[at, :] = e
            out.append(acc + fold(e, mcol[at, :]))
        return tuple(out)

    zero = jnp.zeros((8, protos), F32)
    acc_mine, acc_other = lax.fori_loop(0, rows // LANES, fill, (zero, zero), unroll=True)

    def payload(acc):
        return jnp.concatenate([jnp.sum(acc, axis=0, keepdims=True), count], axis=1)

    slot = here.core * n_plane + here.p
    xy_first[slot] = payload(acc_mine)
    spare[...] = payload(acc_other)

    entered(groups)

    held = xy_first.at[slot]
    for i in range(n_plane - 1):
        send(held, held, f_send.at[0], f_recv.at[0], here.plane[i])
        send(spare, held, f_send.at[0], f_recv.at[0], plane_other[i])
    send(spare, held, f_send.at[0], f_recv.at[0], here.partner)
    z_copy = send(zin.at[other], zx, pair_send.at[0], pair_recv.at[0], here.partner)
    m_copy = send(m_own, ms, pair_send.at[1], pair_recv.at[1], here.partner)

    wait_bytes(ms, pair_recv.at[1])
    for h in range(rows // LANES):
        mcol[rows + h * LANES:rows + (h + 1) * LANES, :] = column_of(ms[h:h + 1, :].astype(F32))
    wait_bytes(zx, pair_recv.at[0])

    def fill_partner(i, _):
        e = jnp.exp(scores(zx[pl.ds(pl.multiple_of(i * LANES, LANES), LANES), :]))
        plan[pl.ds(pl.multiple_of(rows + i * LANES, LANES), LANES), :] = e * e
        return 0

    lax.fori_loop(0, rows // LANES, fill_partner, 0)

    def to_column(t, value):
        held = (z_first if t == 0 else zb.at[t - 1]).at[here.z]
        held[...] = value
        for device in here.column:
            send(held, held, z_send.at[t], z_recv.at[t], device)

    def from_column(t):
        buf = z_first if t == 0 else zb.at[t - 1]
        wait_bytes(buf.at[pl.ds(0, n_z - 1)], z_recv.at[t])
        return jnp.sum(buf[...], axis=0)

    def to_plane(t, value):
        xyb[t, here.p] = value
        held = xyb.at[t, here.p]
        for device in here.plane:
            send(held, held, xy_send.at[t], xy_recv.at[t], device)

    def from_plane(t):
        wait_bytes(xyb.at[t, pl.ds(0, n_plane - 1)], xy_recv.at[t])
        return jnp.sum(xyb[t], axis=0)

    def sweep(a):
        def body(i, acc):
            at = pl.ds(pl.multiple_of(i * LANES, LANES), LANES)
            e = plan[at, :]
            m = mcol[at, :]
            r = jnp.sum(e * a, axis=1, keepdims=True) * m + (1.0 - m)
            return acc + fold(e, m / r)

        acc = lax.fori_loop(0, 2 * rows // LANES, body, zero, unroll=True)
        return jnp.sum(acc, axis=0, keepdims=True)

    wait_bytes(xy_first.at[pl.ds(0, 2 * n_plane - 1)], f_recv.at[0])
    to_column(0, jnp.sum(xy_first[...], axis=0))

    def soften(i, _):
        at = pl.ds(pl.multiple_of(i * 32, 32), 32)
        for view in range(2):
            s = logp[view, at, :]
            s = s - jnp.log(jnp.sum(jnp.exp(s), axis=1, keepdims=True))
            logp[view, at, :] = s
            prob[view, at, :] = jnp.exp(s)
        return 0

    lax.fori_loop(0, rows // 32, soften, 0)
    for k, view in enumerate((mine, other)):
        zt[:, k * rows:(k + 1) * rows] = jnp.transpose(zin[view].astype(F32)).astype(BF16)

    total = from_column(0)
    valid = total[:, protos:]
    for t in (0, 1):
        to_plane(t, sweep(1.0 / (protos * total[:, :protos])))
        to_column(t + 1, from_plane(t))
        total = from_column(t + 1)

    avec[mine] = 1.0 / (protos * total)
    a_held = avec.at[mine]
    a_copy = send(a_held, a_held, pair_send.at[2], pair_recv.at[2], here.partner)

    def weigh(k, view, plan_ref):
        def body(i, _):
            at = pl.ds(pl.multiple_of(i * LANES, LANES), LANES)
            m = mcol[at, :]
            r = jnp.sum(plan_ref[at, :] * avec[view], axis=1, keepdims=True) * m + (1.0 - m)
            bcol[k, at, :] = m / r
            return 0

        lax.fori_loop(0, rows // LANES, body, 0, unroll=True)

    weigh(0, mine, plan)
    wait_bytes(avec.at[other], pair_recv.at[2])
    weigh(1, other, plan_other)
    scale = mcol[0:rows, :] * (0.5 * INV_TEMP) / valid[:, :1]

    def derive(j, _):
        z = here.far_first(j)
        cols = pl.ds(pl.multiple_of(z * block, block), block)
        q_mine = plan[0:rows, cols] * avec[mine, :, cols] * bcol[0]
        q_other = plan_other[:, cols] * avec[other, :, cols] * bcol[1]
        q_out[mine, :, cols] = q_mine
        q_out[other, :, cols] = q_other
        g = jnp.concatenate([((prob[mine, :, cols] - q_other) * scale).astype(BF16),
                             ((prob[other, :, cols] - q_mine) * scale).astype(BF16)], axis=0)
        grad[:, cols] = g
        d = lax.dot_general(zt[...], g, (((1,), (0,)), ((), ())), preferred_element_type=F32)
        part[z] = d.reshape(part.shape[1:])
        send(part.at[z, other], inbox.at[z], c_send.at[j], c_recv.at[j], here.partner)
        return 0

    def spread(j, _):
        z = here.far_first(j)
        wait_bytes(inbox.at[z], c_recv.at[j])
        half[z] = part[z, mine] + inbox[z]
        rs[here.p, z] = half[z, here.p]
        for i in range(n_plane - 1):
            send(half.at[z, here.plane_p[i]], rs.at[here.p, z], r_send.at[j], r_recv.at[j], here.plane[i])
        return 0

    lag = min(3, n_z)
    lax.fori_loop(0, lag, derive, 0)

    def both(j, _):
        derive(j, 0)
        return spread(j - lag, 0)

    lax.fori_loop(lag, n_z, both, 0)
    lax.fori_loop(n_z - lag, n_z, spread, 0)
    q_copy = pltpu.make_async_copy(q_out, q_res, out_sem.at[0])
    q_copy.start()

    def lose(i, acc):
        at = pl.ds(pl.multiple_of(i * 32, 32), 32)
        pair = q_out[1, at, :] * logp[0, at, :] + q_out[0, at, :] * logp[1, at, :]
        return acc + jnp.sum(pair.reshape(4, 8, protos), axis=0)

    loss = jnp.sum(lax.fori_loop(0, rows // 32, lose, zero), keepdims=True)
    lpair[here.core] = jnp.broadcast_to(loss, (1, LANES)) * (-0.5) / valid
    lheld = lpair.at[here.core]
    send(lheld, lheld, l_send.at[0], l_recv.at[0], here.partner)

    def descend(i, _):
        at = pl.ds(pl.multiple_of(i * LANES, LANES), LANES)
        for k, view in enumerate((mine, other)):
            g = grad[pl.ds(pl.multiple_of(k * rows + i * LANES, LANES), LANES), :]
            dz_out[view, at, :] = jnp.dot(g, cbuf[...], preferred_element_type=F32)
        return 0

    lax.fori_loop(0, rows // LANES, descend, 0)
    dz_copy = pltpu.make_async_copy(dz_out, dz_res, out_sem.at[1])
    dz_copy.start()

    wait_bytes(lpair.at[0], l_recv.at[0])
    lxy[here.p] = lpair[0] + lpair[1]
    lheld = lxy.at[here.p]
    for device in here.plane:
        send(lheld, lheld, l_send.at[1], l_recv.at[1], device)

    def gather(j, _):
        z = here.far_first(j)
        wait_bytes(rs.at[pl.ds(0, n_plane - 1), z], r_recv.at[j])
        tot[z] = jnp.sum(rs[:, z], axis=0)

        @pl.when(j < n_z - 1)
        def _():
            send(tot.at[z], zrs.at[here.z], t_send.at[j], t_recv.at[0], here.at(z, here.p, here.core))

        return 0

    lax.fori_loop(0, n_z, gather, 0)
    wait_bytes(lxy.at[pl.ds(0, n_plane - 1)], l_recv.at[1])
    lz[here.z] = jnp.sum(lxy[...], axis=0)
    lheld = lz.at[here.z]
    for device in here.column:
        send(lheld, lheld, l_send.at[2], l_recv.at[2], device)

    zrs[here.z] = tot[here.z]
    wait_bytes(zrs.at[pl.ds(0, n_z - 1)], t_recv.at[0])
    full[here.z, here.p] = jnp.sum(zrs[...], axis=0)

    def near_first(j):
        return here.far_first(n_z - 1 - j)

    held = full.at[here.z, here.p]
    for device in here.column:
        send(held, held, g_send.at[0], g_recv.at[here.z], device)

    def forward(j, _):
        z = near_first(j)
        held = full.at[z, here.p]

        @pl.when(j > 0)
        def _():
            wait_bytes(held, g_recv.at[z])

        for i in range(n_plane - 1):
            send(held, held, x_send.at[j], x_recv.at[j], here.plane[i])
        return 0

    lax.fori_loop(0, n_z, forward, 0)

    def drain(j, _):
        z = near_first(j)
        wait_bytes(inbox.at[z], c_send.at[j])
        wait_bytes(half.at[z, pl.ds(0, n_plane - 1)], r_send.at[j])

        @pl.when(j < n_z - 1)
        def _():
            wait_bytes(tot.at[z], t_send.at[j])

        return 0

    lax.fori_loop(0, n_z, drain, 0)
    z_copy.wait_send()
    m_copy.wait_send()
    a_copy.wait_send()
    wait_bytes(xy_first.at[pl.ds(0, 2 * n_plane - 1)], f_send.at[0])
    wait_bytes(z_first.at[pl.ds(0, n_z - 1)], z_send.at[0])
    for t in (0, 1):
        wait_bytes(xyb.at[t, pl.ds(0, n_plane - 1)], xy_send.at[t])
        wait_bytes(zb.at[t, pl.ds(0, n_z - 1)], z_send.at[t + 1])
    q_copy.wait()
    dz_copy.wait()

    def hand_over(j, which):
        z = near_first(j)
        return pltpu.make_async_copy(
            flip.at[which, z],
            dc_res.at[pl.ds(pl.multiple_of(z * block, block), block), pl.ds(pl.multiple_of(which * LANES, LANES), LANES)],
            out_sem.at[2 + which * n_z + j])

    def cross(j, _):
        z = near_first(j)
        wait_bytes(full.at[z, pl.ds(0, n_plane - 1)], x_recv.at[j])
        flip[mine, z] = jnp.transpose(full[z].reshape(LANES, block))
        held = flip.at[mine, z]
        send(held, held, d_send.at[j], d_recv.at[j], here.partner)
        hand_over(j, mine).start()
        return 0

    lax.fori_loop(0, n_z, cross, 0)

    wait_bytes(lz.at[pl.ds(0, n_z - 1)], l_recv.at[2])
    loss_out[...] = jnp.sum(lz[...], axis=0)
    wait_bytes(lpair.at[0], l_send.at[0])
    wait_bytes(lxy.at[pl.ds(0, n_plane - 1)], l_send.at[1])
    wait_bytes(lz.at[pl.ds(0, n_z - 1)], l_send.at[2])
    wait_bytes(full.at[0, pl.ds(0, n_z - 1)], g_send.at[0])

    def finish(j, _):
        z = near_first(j)
        wait_bytes(flip.at[other, z], d_recv.at[j])
        hand_over(j, other).start()
        wait_bytes(half.at[z, pl.ds(0, n_plane - 1)], x_send.at[j])
        wait_bytes(flip.at[mine, z], d_send.at[j])
        hand_over(j, mine).wait()
        return 0

    lax.fori_loop(0, n_z, finish, 0)

    def settle(j, _):
        hand_over(j, other).wait()
        return 0

    lax.fori_loop(0, n_z, settle, 0)


def whole_step(dims, view_one, view_two, protos, mask):
    rows, depth = view_one.shape
    count = protos.shape[0]
    width = count + LANES
    n_plane, n_z = dims[0] * dims[1], dims[2]
    block = count // n_z
    tile = (LANES // n_plane, block)
    vmem = pl.BlockSpec(memory_space=pltpu.VMEM)
    hbm = pl.BlockSpec(memory_space=pltpu.HBM)
    anywhere = pl.BlockSpec(memory_space=pl.ANY)
    dma, mem = pltpu.SemaphoreType.DMA, pltpu.VMEM
    return pl.pallas_call(
        functools.partial(step_kernel, dims),
        out_shape=(mem((2, rows, count), F32), mem((2, rows, depth), F32), mem((count, depth), F32), mem((1, LANES), F32)),
        in_specs=[hbm] * 4,
        out_specs=(anywhere,) * 3 + (vmem,),
        scratch_shapes=[
            mem((2, rows, count), F32),
            mem((2, rows, depth), F32),
            mem((2, rows, depth), BF16),
            mem((count, depth), BF16),
            mem((rows, depth), BF16),
            mem((rows // LANES, LANES), jnp.int32),
            mem((rows // LANES, LANES), jnp.int32),
            mem((2 * rows, 1), F32),
            mem((2, rows, 1), F32),
            mem((2, 1, count), F32),
            mem((2 * rows, count), F32),
            mem((rows, count), F32),
            mem((2, rows, count), F32),
            mem((2, rows, count), F32),
            mem((2 * rows, count), BF16),
            mem((depth, 2 * rows), BF16),
            mem((2 * n_plane, 1, width), F32),
            mem((1, width), F32),
            mem((2, n_plane, 1, width - LANES), F32),
            mem((n_z, 1, width), F32),
            mem((2, n_z, 1, width - LANES), F32),
            mem((n_z, 2, n_plane) + tile, F32),
            mem((n_z, n_plane) + tile, F32),
            mem((n_z, n_plane) + tile, F32),
            mem((n_plane, n_z) + tile, F32),
            mem((n_z,) + tile, F32),
            mem((n_z,) + tile, F32),
            mem((n_z, n_plane) + tile, F32),
            mem((2, n_z, block, LANES), F32),
            mem((2, 1, LANES), F32),
            mem((n_plane, 1, LANES), F32),
            mem((n_z, 1, LANES), F32),
            dma((4,)), dma((2 + 2 * n_z,)),
            dma((3,)), dma((3,)),
            dma((1,)), dma((1,)),
            dma((2,)), dma((2,)),
            dma((3,)), dma((3,)),
            dma((n_z,)), dma((n_z,)),
            dma((n_z,)), dma((n_z,)),
            dma((n_z,)), dma((1,)),
            dma((1,)), dma((n_z,)),
            dma((n_z,)), dma((n_z,)),
            dma((n_z,)), dma((n_z,)),
            dma((3,)), dma((3,)),
        ],
        compiler_params=pltpu.CompilerParams(collective_id=0, has_side_effects=True, vmem_limit_bytes=32 << 20),
        name="whole_step",
    )(*(pltpu.with_memory_space_constraint(x, pltpu.HBM)
        for x in (view_one, view_two, protos, mask.reshape(rows // LANES, LANES))))


def deliver_kernel(q_ref, dz_ref, dc_ref, loss_ref, q1, q2, dz1, dz2, dc, loss, sem):
    loss[...] = loss_ref[:, :1]
    moves = [(q_ref.at[0], q1), (q_ref.at[1], q2), (dz_ref.at[0], dz1), (dz_ref.at[1], dz2), (dc_ref, dc)]
    copies = [pltpu.make_async_copy(src, dst, sem.at[i]) for i, (src, dst) in enumerate(moves)]
    for copy in copies:
        copy.start()
    for copy in copies:
        copy.wait()


def deliver(q, dz, dc, loss):
    vmem = pl.BlockSpec(memory_space=pltpu.VMEM)
    hbm = pl.BlockSpec(memory_space=pltpu.HBM)
    shapes = [q.shape[1:]] * 2 + [dz.shape[1:]] * 2 + [dc.shape, (1, 1)]
    return pl.pallas_call(
        deliver_kernel,
        out_shape=[jax.ShapeDtypeStruct(shape, F32) for shape in shapes],
        in_specs=[pl.BlockSpec(memory_space=pl.ANY)] * 3 + [vmem],
        out_specs=[hbm] * 5 + [vmem],
        scratch_shapes=[pltpu.SemaphoreType.DMA((5,))],
        compiler_params=pltpu.CompilerParams(vmem_limit_bytes=8 << 20),
        name="deliver",
    )(q, dz, dc, loss)


def solution(mesh):
    dims = torus(mesh.size)

    def local_step(view_one, view_two, protos, valid_mask):
        q, dz, dc, loss = whole_step(dims, view_one, view_two, protos, valid_mask)
        q1, q2, dz1, dz2, dc, loss = deliver(q, dz, dc, loss)
        return q1, q2, loss[0, 0], dz1, dz2, dc

    return jax.shard_map(
        local_step,
        mesh=mesh,
        in_specs=(P("data", None), P("data", None), P(None, None), P("data")),
        out_specs=(P("data", None), P("data", None), P(), P("data", None), P("data", None), P(None, None)),
        check_vma=False,
    )
```
